64 devices in a mesh: dp: 8 (over x, y, core), sp: 8 (over z).
Axes of the slice: x: 2, y: 2, z: 8, core: 2. Of those that a mesh axis runs over, the one named last changes fastest.
The devices are a block of a 4x4x8 slice.
Arguments:
- x: bfloat16 [32768, 5120], P(('dp', 'sp')), parts along dimension 0
- gain: bfloat16 [5120], replicated
- wq: bfloat16 [5120, 4096], replicated
- wk: bfloat16 [5120, 1024], replicated
- wv: bfloat16 [5120, 1024], replicated
- wo: bfloat16 [4096, 5120], replicated
Outputs:
- output: bfloat16 [32768, 5120], P(('dp', 'sp')), parts along dimension 0
There are 8 independent parts. The reference program is written for one: setup_inputs(seed, part) draws one part's arguments, and reference() takes and returns one part's arrays. A program takes and returns all parts, laid end to end along the dimension named above; an argument that names none is the same for every part.
All inputs are finite; a program needn't handle non-finite values.
Results may differ from the reference program's by a relative error of at most 0.012.
Values are sent between devices in bfloat16 or wider.
A program may use at most 768 MiB of HBM per device.

```python
import jax
import jax.numpy as jnp
from jax import lax

ROWS = 4096
D = 5120
HEADS = 32
KV_HEADS = 8
HEAD = 128
THETA = 10000


def setup_inputs(seed: int = 0, part: int = 0) -> dict:
    kx, kn, kq, kk, kv, ko = jax.random.split(jax.random.key(seed), 6)

    def weights(key, rows, columns):
        return jax.random.normal(key, (rows, columns), jnp.float32) * rows**-0.5

    drawn = {
        "x": jax.random.normal(jax.random.fold_in(kx, part), (ROWS, D), jnp.float32),
        "gain": 1 + 0.1 * jax.random.normal(kn, (D,), jnp.float32),
        "wq": 2 * weights(kq, D, HEADS * HEAD),
        "wk": 2 * weights(kk, D, KV_HEADS * HEAD),
        "wv": 4 * weights(kv, D, KV_HEADS * HEAD),
        "wo": weights(ko, HEADS * HEAD, D),
    }
    return {k: v.astype(jnp.bfloat16) for k, v in drawn.items()}


def normed(x, gain):
    wide = x.astype(jnp.float32)
    scale = lax.rsqrt(jnp.mean(wide * wide, -1, keepdims=True) + 1e-6)
    return (wide * scale * gain.astype(jnp.float32)).astype(jnp.bfloat16)


def turned(t, place, theta):
    half = t.shape[-1] // 2
    angle = place.astype(jnp.float32)[:, None] * theta ** (-jnp.arange(half, dtype=jnp.float32) / half)
    cos, sin = jnp.cos(angle)[:, None], jnp.sin(angle)[:, None]
    a, b = t[..., :half].astype(jnp.float32), t[..., half:].astype(jnp.float32)
    return jnp.concatenate([a * cos - b * sin, b * cos + a * sin], -1).astype(jnp.bfloat16)


def matmul(a, w):
    return jnp.dot(a, w, preferred_element_type=jnp.float32).astype(jnp.bfloat16)


def einsum(form, a, b):
    return jnp.einsum(form, a.astype(jnp.float32), b.astype(jnp.float32))


def attention(q, k, v):
    scores = einsum("tgsd,ugd->gstu", q, k) * q.shape[-1] ** -0.5
    token = jnp.arange(q.shape[0])
    scores = jnp.where(token[:, None] >= token, scores, -jnp.inf)
    weights = jax.nn.softmax(scores, -1).astype(jnp.bfloat16)
    return einsum("gstu,ugd->tgsd", weights, v).astype(jnp.bfloat16)


def reference(x, gain, wq, wk, wv, wo):
    a, place = normed(x, gain), jnp.arange(ROWS)
    q = turned(matmul(a, wq).reshape(ROWS, HEADS, HEAD), place, THETA).reshape(ROWS, KV_HEADS, -1, HEAD)
    k = turned(matmul(a, wk).reshape(ROWS, KV_HEADS, HEAD), place, THETA)
    v = matmul(a, wv).reshape(ROWS, KV_HEADS, HEAD)
    seen = attention(q, k, v).reshape(ROWS, HEADS * HEAD)
    return (x.astype(jnp.float32) + jnp.dot(seen, wo, preferred_element_type=jnp.float32)).astype(jnp.bfloat16)
```

```python
import functools

import jax
import jax.numpy as jnp
from jax import lax
from jax.experimental import pallas as pl
from jax.experimental.pallas import tpu as pltpu
from jax.sharding import PartitionSpec as P

HEAD = 128
THETA = 10000
LOG2E = 1.4426950408889634
HIDDEN = -2e30
TILE = 512
F32, BF16 = jnp.float32, jnp.bfloat16


def _dot(a, b, ca, cb):
    return lax.dot_general(a, b, (((ca,), (cb,)), ((), ())), preferred_element_type=F32)


def _kernel(n, g, x_ref, gain_ref, cos_ref, sin_ref, wq_ref, wk_ref, wv_ref, wo_ref, y_ref,
            a_s, y_s, q_s, kv_s, mix_s, top_s, o_s, w_s, w_sem, x_sem, y_sem, sr_sem, sl_sem, rr_sem, rl_sem):
    own, depth = x_ref.shape
    kv = kv_s.shape[1]
    half, near = n // 2, n // 2 - 1
    parts = depth // TILE
    scale = HEAD**-0.5
    e2 = scale * LOG2E
    me = lax.axis_index("sp")
    right, left = lax.rem(me + 1, n), lax.rem(me + n - 1, n)

    def column_tile(ref, t, slot):
        return pltpu.make_async_copy(ref.at[:, pl.ds(pl.multiple_of(t * TILE, TILE), TILE)], w_s.at[slot], w_sem.at[slot])

    def fetch_row_tile(h, slot):
        for c in range(parts):
            pltpu.make_async_copy(wo_ref.at[pl.ds(pl.multiple_of(h * TILE, TILE), TILE), c * TILE : (c + 1) * TILE],
                                  w_s.at[slot, c * TILE : (c + 1) * TILE, :], w_sem.at[slot]).start()

    def wait_tile(slot):
        column_tile(wq_ref, 0, slot).wait()

    column_tile(wk_ref, 0, 0).start()
    for c in range(parts):
        pltpu.make_async_copy(x_ref.at[:, c * TILE : (c + 1) * TILE], w_s.at[1, c * TILE : (c + 1) * TILE, :], x_sem).start()

    barrier = pltpu.get_barrier_semaphore()
    for neighbour in (left, right):
        pl.semaphore_signal(barrier, inc=1, device_id={"sp": neighbour}, device_id_type=pl.DeviceIdType.MESH)
    pl.semaphore_wait(barrier, 2)

    pltpu.make_async_copy(wq_ref.at[:, :TILE], w_s.at[1], x_sem).wait()

    def piece(c):
        return pl.ds(pl.multiple_of(c * TILE, TILE), TILE)

    def squares(c, total):
        wide = w_s[1, piece(c), :].astype(F32)
        return total + (wide * wide).sum(-1, keepdims=True)

    total = lax.fori_loop(0, parts, squares, jnp.zeros((own, 1), F32))
    by = lax.rsqrt(total / depth + 1e-6)

    def norm(c, _):
        wide = w_s[1, piece(c), :].astype(F32)
        a_s[:, piece(c)] = (wide * by * gain_ref[:, piece(c)].astype(F32)).astype(BF16)
        y_s[c] = wide

    lax.fori_loop(0, parts, norm, None)
    column_tile(wv_ref, 0, 1).start()

    def right_copy(b, h, at):
        return pltpu.make_async_remote_copy(kv_s.at[b, h], kv_s.at[b, h], sr_sem.at[at, h], rr_sem.at[at, h],
                                            device_id={"sp": right}, device_id_type=pl.DeviceIdType.MESH)

    def left_copy(b, h, at_send, at_receive):
        return pltpu.make_async_remote_copy(kv_s.at[b, h], kv_s.at[b, h], sl_sem.at[at_send, h], rl_sem.at[at_receive, h],
                                            device_id={"sp": left}, device_id_type=pl.DeviceIdType.MESH)

    def comes_right(i, s, h):
        return ((s <= near) & (s <= i)) | ((s == half) & (i == n - 1) & (h >= kv // 2))

    def left_block(i, u):
        return jnp.where(i >= half, u - 1, i + u)

    def comes_left(i, u, h):
        count = jnp.where(i >= half, i - near, near - i)
        return (u <= count) & ((left_block(i, u) < near) | (h < kv // 2))

    def goes_left(i, b):
        return (i < half) | (i - 1 >= b + half)

    def left_place(i, b):
        to = lax.rem(i + n - 1, n)
        return jnp.where(to >= half, b, b - to - 1)

    def send_right(s, h, do):
        @pl.when((me < n - 1) & comes_right(me + 1, s + 1, h))
        def _():
            do(right_copy(jnp.maximum(me - s, 0), h, s))

    def send_left(u, h, do):
        b = jnp.clip(left_block(me, u), 0, n - 1) if not (isinstance(u, int) and u == 0) else me
        own_block = isinstance(u, int) and u == 0
        ok = (me < half) & ((me < near) | (h < kv // 2)) if own_block else comes_left(me, u, h) & goes_left(me, b)

        @pl.when(ok)
        def _():
            do(left_copy(b, h, u, jnp.clip(left_place(me, b), 0, half - 1)))

    def start(copy):
        copy.start()

    def send_own(h):
        send_right(0, h, start)
        send_left(0, h, start)

    def turned(t, c):
        return (t * cos_ref[...] + pltpu.roll(t, HEAD // 2, 1) * sin_ref[...]).astype(BF16)

    def project(slot):
        return _dot(a_s[...], w_s[slot], 1, 0).astype(BF16)

    per_tile = TILE // HEAD

    def keys_values(i, _):
        wait_tile(0)
        t = project(0)
        for m in range(per_tile):
            kv_s[me, i * per_tile + m, 0] = turned(t[:, m * HEAD : (m + 1) * HEAD].astype(F32), m)

        @pl.when(i == 0)
        def _():
            column_tile(wk_ref, 1, 0).start()

        @pl.when(i == 1)
        def _():
            column_tile(wq_ref, 0, 0).start()

        wait_tile(1)
        t = project(1)
        for m in range(per_tile):
            kv_s[me, i * per_tile + m, 1] = t[:, m * HEAD : (m + 1) * HEAD]

        @pl.when(i == 0)
        def _():
            column_tile(wv_ref, 1, 1).start()

        for m in range(per_tile):
            send_own(i * per_tile + m)

    lax.fori_loop(0, kv // per_tile, keys_values, None)

    ones = jnp.ones((8, own), BF16)

    def attend(h, b, first):
        keys, values = kv_s[b, h, 0], jnp.concatenate([kv_s[b, h, 1].T, ones], axis=0)
        scores = [_dot(keys, q_s[h, m * own : (m + 1) * own, :], 1, 1) for m in range(g)]
        if first:
            seen = lax.broadcasted_iota(jnp.int32, (own, own), 1) >= lax.broadcasted_iota(jnp.int32, (own, own), 0)
        weights, keeps = [], []
        for m, s in enumerate(scores):
            at = slice(m * own, (m + 1) * own)
            if first:
                s = jnp.where(seen, s, HIDDEN)
                top = s.max(axis=0, keepdims=True)
            else:
                old = top_s[h, :, at]
                top = jnp.maximum(old, s.max(axis=0, keepdims=True))
                keeps.append(jnp.exp2((old - top) * e2))
            top_s[h, :, at] = top
            weights.append(jnp.exp2((s - top) * e2).astype(BF16))
        for m, p in enumerate(weights):
            at = slice(m * own, (m + 1) * own)
            new = _dot(values, p, 1, 0)
            mix_s[h, :, at] = new if first else mix_s[h, :, at] * keeps[m] + new

    def arrivals(r, h):
        @pl.when(comes_right(me, r, h))
        def _():
            right_copy(jnp.maximum(me - r, 0), h, r - 1).wait_recv()

        if not isinstance(r, int) or r < half:
            send_right(r, h, start)

        @pl.when(comes_right(me, r, h))
        def _():
            attend(h, jnp.maximum(me - r, 0), False)

        b = jnp.clip(left_block(me, r), 0, n - 1)

        @pl.when(comes_left(me, r, h))
        def _():
            left_copy(b, h, 0, r - 1).wait_recv()

        if not isinstance(r, int) or r < half:
            send_left(r, h, start)

        @pl.when(comes_left(me, r, h) & (me >= half))
        def _():
            attend(h, b, False)

    def queries(h, _):
        slot = lax.rem(h, 2)
        wait_tile(slot)

        @pl.when(h < kv - 1)
        def _():
            column_tile(wq_ref, jnp.minimum(h + 1, kv - 1), 1 - slot).start()

        @pl.when(h == kv - 1)
        def _():
            fetch_row_tile(0, 0)

        t = project(slot)
        for m in range(g):
            q_s[h, m * own : (m + 1) * own, :] = turned(t[:, m * HEAD : (m + 1) * HEAD].astype(F32), m)
        attend(h, me, True)
        arrivals(1, h)

    lax.fori_loop(0, kv, queries, None)

    def middle(i, _):
        arrivals(2 + lax.div(i, kv), lax.rem(i, kv))

    lax.fori_loop(0, (half - 2) * kv, middle, None)

    def head_at(i):
        return lax.div(i, 2) + (kv // 2) * lax.rem(i, 2)

    def last(i, _):
        slot, h = lax.rem(i, 2), head_at(i)
        arrivals(half, h)
        for m in range(g):
            at = slice(m * own, (m + 1) * own)
            o = mix_s[h, :HEAD, at] * (1 / mix_s[h, HEAD : HEAD + 1, at])
            o_s[:, m * HEAD : (m + 1) * HEAD] = o.T.astype(BF16)
        wait_tile(slot)

        @pl.when(i < kv - 1)
        def _():
            fetch_row_tile(head_at(jnp.minimum(i + 1, kv - 1)), 1 - slot)

        def out(c, _):
            for m in range(2):
                y_s[2 * c + m] += _dot(o_s[...], w_s[slot, piece(2 * c + m), :], 1, 0)

        lax.fori_loop(0, parts // 2, out, None)

    lax.fori_loop(0, kv, last, None)

    def out_copy(c):
        return pltpu.make_async_copy(w_s.at[0, piece(c), :], y_ref.at[:, piece(c)], y_sem.at[c])

    def store(c, _):
        w_s[0, piece(c), :] = y_s[c].astype(BF16)
        out_copy(c).start()

    lax.fori_loop(0, parts, store, None)

    def settle(i, _):
        s, h = lax.div(i, kv), lax.rem(i, kv)
        send_right(s, h, lambda copy: copy.wait_send())

        @pl.when(s > 0)
        def _():
            send_left(s, h, lambda copy: copy.wait_send())

    def settle_own(h, _):
        send_left(0, h, lambda copy: copy.wait_send())

    lax.fori_loop(0, half * kv, settle, None)
    lax.fori_loop(0, kv, settle_own, None)

    def stored(c, _):
        out_copy(c).wait()

    lax.fori_loop(0, parts, stored, None)


def solution(mesh):
    n = mesh.shape["sp"]

    def step(x, gain, wq, wk, wv, wo):
        own, depth = x.shape
        kv = wk.shape[1] // HEAD
        g = wq.shape[1] // wk.shape[1]
        half = HEAD // 2
        place = lax.axis_index("sp") * own + jnp.arange(own)
        angle = place.astype(F32)[:, None] * THETA ** (-jnp.arange(half, dtype=F32) / half)
        cos, sin = jnp.cos(angle), jnp.sin(angle)
        cos, sin = jnp.concatenate([cos, cos], 1), jnp.concatenate([-sin, sin], 1)
        hbm, vmem = pl.BlockSpec(memory_space=pl.ANY), pl.BlockSpec(memory_space=pltpu.VMEM)
        dma = pltpu.SemaphoreType.DMA
        return pl.pallas_call(
            functools.partial(_kernel, n, g),
            out_shape=jax.ShapeDtypeStruct((own, depth), BF16),
            in_specs=[hbm, vmem, vmem, vmem, hbm, hbm, hbm, hbm],
            out_specs=hbm,
            scratch_shapes=[
                pltpu.VMEM((own, depth), BF16),
                pltpu.VMEM((depth // TILE, own, TILE), F32),
                pltpu.VMEM((kv, g * own, HEAD), BF16),
                pltpu.VMEM((n, kv, 2, own, HEAD), BF16),
                pltpu.VMEM((kv, HEAD + 8, g * own), F32),
                pltpu.VMEM((kv, 1, g * own), F32),
                pltpu.VMEM((own, g * HEAD), BF16),
                pltpu.VMEM((2, depth, TILE), BF16),
                dma((2,)), dma, dma((depth // TILE,)),
                dma((n // 2, kv)), dma((n // 2, kv)), dma((n // 2, kv)), dma((n // 2, kv)),
            ],
            compiler_params=pltpu.CompilerParams(collective_id=0, has_side_effects=True, vmem_limit_bytes=67_043_328),
            cost_estimate=pl.CostEstimate(flops=2 * own * depth * (wq.shape[1] * 2 + wk.shape[1] * 2), bytes_accessed=2 * (2 * wq.size + 2 * wk.size), transcendentals=0),
        )(x, gain[None], cos, sin, wq, wk, wv, wo)

    tokens, whole = P(("dp", "sp"), None), P(None, None)
    return jax.shard_map(
        step,
        mesh=mesh,
        in_specs=(tokens, P(None), whole, whole, whole, whole),
        out_specs=tokens,
        check_vma=False,
    )
```

```python
import functools

import jax
import jax.numpy as jnp
import numpy as np
from jax import lax
from jax.experimental import pallas as pl
from jax.experimental.pallas import tpu as pltpu
from jax.sharding import PartitionSpec as P

HEAD = 128
THETA = 10000
LOG2E = 1.4426950408889634
HIDDEN = -2e30
TILE = 512
F32, BF16 = jnp.float32, jnp.bfloat16


def _dot(a, b, ca, cb):
    return lax.dot_general(a, b, (((ca,), (cb,)), ((), ())), preferred_element_type=F32)


def _kernel(n, g, x_ref, gain_ref, turn_ref, wq_ref, wk_ref, wv_ref, wo_ref, y_ref,
            cos_s, sin_s, a_s, y_s, q_s, kv_s, mix_s, top_s, o_s, w_s, w_sem, x_sem, y_sem, sr_sem, sl_sem, rr_sem, rl_sem):
    own, depth = x_ref.shape
    kv = kv_s.shape[1]
    team = kv // 2
    half, near = n // 2, n // 2 - 1
    parts = depth // TILE
    scale = HEAD**-0.5
    e2 = scale * LOG2E
    me = lax.axis_index("sp")
    right, left = lax.rem(me + 1, n), lax.rem(me + n - 1, n)

    def column_tile(ref, t, slot):
        return pltpu.make_async_copy(ref.at[:, pl.ds(pl.multiple_of(t * TILE, TILE), TILE)], w_s.at[slot], w_sem.at[slot])

    def fetch_row_tile(h, slot):
        for c in range(parts):
            pltpu.make_async_copy(wo_ref.at[pl.ds(pl.multiple_of(h * TILE, TILE), TILE), c * TILE : (c + 1) * TILE],
                                  w_s.at[slot, c * TILE : (c + 1) * TILE, :], w_sem.at[slot]).start()

    def fetch_pair_tile(i, slot):
        cols = pl.ds(pl.multiple_of(i * (TILE // 2), TILE // 2), TILE // 2)
        pltpu.make_async_copy(wk_ref.at[:, cols], w_s.at[slot, :, : TILE // 2], w_sem.at[slot]).start()
        pltpu.make_async_copy(wv_ref.at[:, cols], w_s.at[slot, :, TILE // 2 :], w_sem.at[slot]).start()

    def wait_tile(slot):
        column_tile(wq_ref, 0, slot).wait()

    fetch_pair_tile(0, 0)
    for c in range(parts):
        pltpu.make_async_copy(x_ref.at[:, c * TILE : (c + 1) * TILE], w_s.at[1, c * TILE : (c + 1) * TILE, :], x_sem).start()

    barrier = pltpu.get_barrier_semaphore()
    for neighbour in (left, right):
        pl.semaphore_signal(barrier, inc=1, device_id={"sp": neighbour}, device_id_type=pl.DeviceIdType.MESH)

    at = lax.broadcasted_iota(jnp.int32, (own, HEAD), 0) + me * own
    angle = at.astype(F32) * turn_ref[...]
    sine = jnp.sin(angle)
    cos_s[...] = jnp.cos(angle)
    sin_s[...] = jnp.where(lax.broadcasted_iota(jnp.int32, (own, HEAD), 1) < HEAD // 2, -sine, sine)
    pl.semaphore_wait(barrier, 2)

    pltpu.make_async_copy(wq_ref.at[:, :TILE], w_s.at[1], x_sem).wait()

    def piece(c):
        return pl.ds(pl.multiple_of(c * TILE, TILE), TILE)

    def squares(c, total):
        wide = w_s[1, piece(c), :].astype(F32)
        return total + (wide * wide).sum(-1, keepdims=True)

    total = lax.fori_loop(0, parts, squares, jnp.zeros((own, 1), F32))
    by = lax.rsqrt(total / depth + 1e-6)

    def norm(c, _):
        wide = w_s[1, piece(c), :].astype(F32)
        a_s[:, piece(c)] = (wide * by * gain_ref[:, piece(c)].astype(F32)).astype(BF16)
        y_s[c] = wide

    lax.fori_loop(0, parts, norm, None)
    fetch_pair_tile(1, 1)

    def right_copy(b, h, at):
        return pltpu.make_async_remote_copy(kv_s.at[b, h], kv_s.at[b, h], sr_sem.at[at, h], rr_sem.at[at, h],
                                            device_id={"sp": right}, device_id_type=pl.DeviceIdType.MESH)

    def left_copy(b, h, at):
        return pltpu.make_async_remote_copy(kv_s.at[b, h], kv_s.at[b, h], sl_sem.at[at, h], rl_sem.at[at, h],
                                            device_id={"sp": left}, device_id_type=pl.DeviceIdType.MESH)

    def by_right(h):
        return lax.rem(h, team) >= team // 2

    def comes_right(i, s, h):
        return ((s <= near) & (s <= i)) | ((s == half) & (i >= half) & by_right(h))

    def comes_left(i, s, h):
        b = lax.rem(i + s, n)
        whole = (s <= near) & (b < near)
        return (i != near) & (b < half) & (whole | ((s <= half) & ~by_right(h)))

    def send_right(s, h, do, also=None):
        ok = (me < n - 1) & comes_right(me + 1, s + 1, h)

        @pl.when(ok if also is None else ok & also)
        def _():
            do(right_copy(jnp.maximum(me - s, 0), h, s))

    def send_left(s, h, do, also=None):
        ok = comes_left(left, s + 1, h)

        @pl.when(ok if also is None else ok & also)
        def _():
            do(left_copy(lax.rem(me + s, n), h, s))

    def start(copy):
        copy.start()

    def send_own(h):
        send_right(0, h, start)
        send_left(0, h, start)

    def turned(t):
        return (t * cos_s[...] + pltpu.roll(t, HEAD // 2, 1) * sin_s[...]).astype(BF16)

    def project(slot):
        return _dot(a_s[...], w_s[slot], 1, 0).astype(BF16)

    pair = TILE // HEAD // 2

    def keys_values(i, _):
        slot = lax.rem(i, 2)
        wait_tile(slot)
        t = project(slot)
        for m in range(pair):
            h = i * pair + m
            kv_s[me, h, 0] = turned(t[:, m * HEAD : (m + 1) * HEAD].astype(F32))
            kv_s[me, h, 1] = t[:, (pair + m) * HEAD : (pair + m + 1) * HEAD]

        @pl.when(i < kv // pair - 2)
        def _():
            fetch_pair_tile(jnp.minimum(i + 2, kv // pair - 1), slot)

        @pl.when(i == kv // pair - 2)
        def _():
            column_tile(wq_ref, 0, 0).start()

        for m in range(pair):
            send_own(i * pair + m)

    lax.fori_loop(0, kv // pair, keys_values, None)

    ones = jnp.ones((8, own), BF16)

    def attend(h, b, first):
        keys, values = kv_s[b, h, 0], jnp.concatenate([kv_s[b, h, 1].T, ones], axis=0)
        scores = [_dot(keys, q_s[h, m * own : (m + 1) * own, :], 1, 1) for m in range(g)]
        if first:
            seen = lax.broadcasted_iota(jnp.int32, (own, own), 1) >= lax.broadcasted_iota(jnp.int32, (own, own), 0)
        weights, keeps = [], []
        for m, s in enumerate(scores):
            at = slice(m * own, (m + 1) * own)
            if first:
                s = jnp.where(seen, s, HIDDEN)
                top = s.max(axis=0, keepdims=True)
            else:
                old = top_s[h, :, at]
                top = jnp.maximum(old, s.max(axis=0, keepdims=True))
                keeps.append(jnp.exp2((old - top) * e2))
            top_s[h, :, at] = top
            weights.append(jnp.exp2((s - top) * e2).astype(BF16))
        for m, p in enumerate(weights):
            at = slice(m * own, (m + 1) * own)
            new = _dot(values, p, 1, 0)
            mix_s[h, :, at] = new if first else mix_s[h, :, at] * keeps[m] + new

    last_right, last_left = (me >= near) & (me < n - 1), (me == 0) | (me > half)

    def arrivals(r, h):
        def now(late):
            return None if r != near - 1 else ~late | (h < team)

        @pl.when(comes_right(me, r, h))
        def _():
            right_copy(jnp.maximum(me - r, 0), h, r - 1).wait_recv()

        if r < half:
            send_right(r, h, start, now(last_right))

        @pl.when(comes_right(me, r, h))
        def _():
            attend(h, jnp.maximum(me - r, 0), False)

        b = lax.rem(me + r, n)

        @pl.when(comes_left(me, r, h))
        def _():
            left_copy(b, h, r - 1).wait_recv()

        if r < half:
            send_left(r, h, start, now(last_left))

        @pl.when(comes_left(me, r, h) & (me >= half))
        def _():
            attend(h, b, False)

    def queries(h, _):
        slot = lax.rem(h, 2)
        wait_tile(slot)

        @pl.when(h < kv - 1)
        def _():
            column_tile(wq_ref, jnp.minimum(h + 1, kv - 1), 1 - slot).start()

        @pl.when(h == kv - 1)
        def _():
            fetch_row_tile(0, 0)

        t = project(slot)
        for m in range(g):
            q_s[h, m * own : (m + 1) * own, :] = turned(t[:, m * HEAD : (m + 1) * HEAD].astype(F32))
        attend(h, me, True)
        arrivals(1, h)

    lax.fori_loop(0, kv, queries, None)
    for r in range(2, near):
        lax.fori_loop(0, kv, lambda h, _: arrivals(r, h), None)

    def group(which, _):
        base = which * team

        def middle(i, _):
            h = base + i
            arrivals(near, h)

            @pl.when(which == 0)
            def _():
                kept = jnp.minimum(h + team, kv - 1)
                send_right(near - 1, kept, start, last_right)
                send_left(near - 1, kept, start, last_left)

        lax.fori_loop(0, team, middle, None)

        def head_at(i):
            return base + lax.div(i, 2) + (team // 2) * lax.rem(i, 2)

        def last(i, _):
            slot, h = lax.rem(i, 2), head_at(i)
            arrivals(half, h)
            for m in range(g):
                at = slice(m * own, (m + 1) * own)
                o = mix_s[h, :HEAD, at] * (1 / mix_s[h, HEAD : HEAD + 1, at])
                o_s[:, m * HEAD : (m + 1) * HEAD] = o.T.astype(BF16)
            wait_tile(slot)

            @pl.when(i < team - 1)
            def _():
                fetch_row_tile(head_at(jnp.minimum(i + 1, team - 1)), 1 - slot)

            @pl.when((i == team - 1) & (which == 0))
            def _():
                fetch_row_tile(team, 0)

            def out(c, _):
                for m in range(parts // 2):
                    y_s[parts // 2 * c + m] += _dot(o_s[...], w_s[slot, piece(parts // 2 * c + m), :], 1, 0)

            lax.fori_loop(0, 2, out, None)

        lax.fori_loop(0, team, last, None)

    lax.fori_loop(0, 2, group, None)

    def out_copy(c):
        return pltpu.make_async_copy(w_s.at[0, piece(c), :], y_ref.at[:, piece(c)], y_sem.at[c])

    def store(c, _):
        w_s[0, piece(c), :] = y_s[c].astype(BF16)
        out_copy(c).start()

    lax.fori_loop(0, parts, store, None)

    def settle(i, _):
        s, h = lax.div(i, kv), lax.rem(i, kv)
        send_right(s, h, lambda copy: copy.wait_send())
        send_left(s, h, lambda copy: copy.wait_send())

    lax.fori_loop(0, half * kv, settle, None)

    def stored(c, _):
        out_copy(c).wait()

    lax.fori_loop(0, parts, stored, None)


def solution(mesh):
    n = mesh.shape["sp"]

    def step(x, gain, wq, wk, wv, wo):
        own, depth = x.shape
        kv = wk.shape[1] // HEAD
        g = wq.shape[1] // wk.shape[1]
        half = HEAD // 2
        turn = np.float32(THETA) ** (-np.arange(half, dtype=np.float32) / half)
        turn = jnp.asarray(np.concatenate([turn, turn])[None])
        hbm, vmem = pl.BlockSpec(memory_space=pl.ANY), pl.BlockSpec(memory_space=pltpu.VMEM)
        dma = pltpu.SemaphoreType.DMA
        return pl.pallas_call(
            functools.partial(_kernel, n, g),
            out_shape=jax.ShapeDtypeStruct((own, depth), BF16),
            in_specs=[hbm, vmem, vmem, hbm, hbm, hbm, hbm],
            out_specs=hbm,
            scratch_shapes=[
                pltpu.VMEM((own, HEAD), F32),
                pltpu.VMEM((own, HEAD), F32),
                pltpu.VMEM((own, depth), BF16),
                pltpu.VMEM((depth // TILE, own, TILE), F32),
                pltpu.VMEM((kv, g * own, HEAD), BF16),
                pltpu.VMEM((n, kv, 2, own, HEAD), BF16),
                pltpu.VMEM((kv, HEAD + 8, g * own), F32),
                pltpu.VMEM((kv, 1, g * own), F32),
                pltpu.VMEM((own, g * HEAD), BF16),
                pltpu.VMEM((2, depth, TILE), BF16),
                dma((2,)), dma, dma((depth // TILE,)),
                dma((n // 2, kv)), dma((n // 2, kv)), dma((n // 2, kv)), dma((n // 2, kv)),
            ],
            compiler_params=pltpu.CompilerParams(collective_id=0, has_side_effects=True, vmem_limit_bytes=67_043_328),
            cost_estimate=pl.CostEstimate(flops=2 * own * depth * (wq.shape[1] * 2 + wk.shape[1] * 2), bytes_accessed=2 * (2 * wq.size + 2 * wk.size), transcendentals=0),
        )(x, gain[None], turn, wq, wk, wv, wo)

    tokens, whole = P(("dp", "sp"), None), P(None, None)
    return jax.shard_map(
        step,
        mesh=mesh,
        in_specs=(tokens, P(None), whole, whole, whole, whole),
        out_specs=tokens,
        check_vma=False,
    )
```

```python
import functools

import jax
import jax.numpy as jnp
import numpy as np
from jax import lax
from jax.experimental import pallas as pl
from jax.experimental.pallas import tpu as pltpu
from jax.sharding import PartitionSpec as P

HEAD = 128
THETA = 10000
LOG2E = 1.4426950408889634
HIDDEN = -2e30
TILE = 512
GROUPS = 4
F32, BF16 = jnp.float32, jnp.bfloat16


def _dot(a, b, ca, cb):
    return lax.dot_general(a, b, (((ca,), (cb,)), ((), ())), preferred_element_type=F32)


def _kernel(n, g, groups, x_ref, gain_ref, turn_ref, wq_ref, wk_ref, wv_ref, wo_ref, y_ref,
            cos_s, sin_s, a_s, y_s, q_s, kv_s, mix_s, top_s, o_s, w_s, w_sem, x_sem, y_sem, sr_sem, sl_sem, rr_sem, rl_sem):
    own, depth = x_ref.shape
    kv = kv_s.shape[1]
    team = kv // groups
    half, near = n // 2, n // 2 - 1
    parts = depth // TILE
    scale = HEAD**-0.5
    e2 = scale * LOG2E
    me = lax.axis_index("sp")
    right, left = lax.rem(me + 1, n), lax.rem(me + n - 1, n)

    def column_tile(ref, t, slot):
        return pltpu.make_async_copy(ref.at[:, pl.ds(pl.multiple_of(t * TILE, TILE), TILE)], w_s.at[slot], w_sem.at[slot])

    def fetch_row_tile(h, slot):
        for c in range(parts):
            pltpu.make_async_copy(wo_ref.at[pl.ds(pl.multiple_of(h * TILE, TILE), TILE), c * TILE : (c + 1) * TILE],
                                  w_s.at[slot, c * TILE : (c + 1) * TILE, :], w_sem.at[slot]).start()

    def fetch_pair_tile(i, slot):
        for m in range(TILE // HEAD):
            cols = pl.ds(pl.multiple_of((2 * i + m // 2) * HEAD, HEAD), HEAD)
            pltpu.make_async_copy((wk_ref, wv_ref)[m % 2].at[:, cols], w_s.at[slot, :, m * HEAD : (m + 1) * HEAD], w_sem.at[slot]).start()

    def wait_tile(slot):
        column_tile(wq_ref, 0, slot).wait()

    for c in range(parts):
        pltpu.make_async_copy(x_ref.at[:, c * TILE : (c + 1) * TILE], w_s.at[1, c * TILE : (c + 1) * TILE, :], x_sem).start()
    fetch_pair_tile(0, 0)

    barrier = pltpu.get_barrier_semaphore()
    for neighbour in (left, right):
        pl.semaphore_signal(barrier, inc=1, device_id={"sp": neighbour}, device_id_type=pl.DeviceIdType.MESH)

    at = lax.broadcasted_iota(jnp.int32, (own, HEAD), 0) + me * own
    angle = at.astype(F32) * turn_ref[...]
    sine = jnp.sin(angle)
    cos_s[...] = jnp.cos(angle)
    sin_s[...] = jnp.where(lax.broadcasted_iota(jnp.int32, (own, HEAD), 1) < HEAD // 2, -sine, sine)

    pltpu.make_async_copy(wq_ref.at[:, :TILE], w_s.at[1], x_sem).wait()

    def piece(c):
        return pl.ds(pl.multiple_of(c * TILE, TILE), TILE)

    def squares(c, total):
        wide = w_s[1, piece(c), :].astype(F32)
        return total + (wide * wide).sum(-1, keepdims=True)

    total = lax.fori_loop(0, parts, squares, jnp.zeros((own, 1), F32))
    by = lax.rsqrt(total / depth + 1e-6)

    def norm(c, _):
        wide = w_s[1, piece(c), :].astype(F32)
        a_s[:, piece(c)] = (wide * by * gain_ref[piece(c)].astype(F32)[None]).astype(BF16)
        y_s[c] = wide

    lax.fori_loop(0, parts, norm, None)
    fetch_pair_tile(1, 1)

    pl.semaphore_wait(barrier, 2)

    def remote(b, h, to, send, receive, part):
        rows = slice(None) if part is None else slice(part * own // 2, (part + 1) * own // 2)
        ref = kv_s.at[b, h, :, rows, :]
        return pltpu.make_async_remote_copy(ref, ref, send, receive, device_id={"sp": to}, device_id_type=pl.DeviceIdType.MESH)

    def right_copy(b, h, at, part):
        return remote(b, h, right, sr_sem.at[at, h], rr_sem.at[at, h], part)

    def left_copy(b, h, at, part):
        return remote(b, h, left, sl_sem.at[at, h], rl_sem.at[at, h], part)

    def comes_right(i, s):
        return s <= i if s <= near else i >= half

    def comes_left(i, s):
        b = lax.rem(i + s, n)
        if s > near:
            return False, i >= half
        return (i != near) & (b < near), (i != near) & (b == near)

    def both(ok, also):
        return ok if also is None else ok & also

    def send_right(s, h, do, also=None):
        @pl.when(both((me < n - 1) & comes_right(me + 1, s + 1), also))
        def _():
            do(right_copy(jnp.maximum(me - s, 0), h, s, None if s < near else 1))

    def send_left(s, h, do, also=None):
        whole, part = comes_left(left, s + 1)
        b = lax.rem(me + s, n)
        if whole is not False:
            @pl.when(both(whole, also))
            def _():
                do(left_copy(b, h, s, None))

        @pl.when(both(part, also))
        def _():
            do(left_copy(b, h, s, 0))

    def start(copy):
        copy.start()

    def send_own(h):
        send_right(0, h, start)
        send_left(0, h, start)

    def turned(t):
        return (t * cos_s[...] + pltpu.roll(t, HEAD // 2, 1) * sin_s[...]).astype(BF16)

    def project(slot):
        return _dot(a_s[...], w_s[slot], 1, 0).astype(BF16)

    pair = TILE // HEAD // 2

    def keys_values(i, _):
        slot = lax.rem(i, 2)
        wait_tile(slot)
        for m in range(pair):
            h = i * pair + m
            t = _dot(a_s[...], w_s[slot, :, 2 * m * HEAD : 2 * (m + 1) * HEAD], 1, 0).astype(BF16)
            kv_s[me, h, 0] = turned(t[:, :HEAD].astype(F32))
            kv_s[me, h, 1] = t[:, HEAD:]
            send_own(h)

        @pl.when(i < kv // pair - 2)
        def _():
            fetch_pair_tile(jnp.minimum(i + 2, kv // pair - 1), slot)

        @pl.when(i == kv // pair - 2)
        def _():
            column_tile(wq_ref, 0, 0).start()

    lax.fori_loop(0, kv // pair, keys_values, None)

    ones = jnp.ones((8, own), BF16)

    def attend(h, b, first):
        keys, values = kv_s[b, h, 0], jnp.concatenate([kv_s[b, h, 1].T, ones], axis=0)
        scores = [_dot(keys, q_s[h, m * own : (m + 1) * own, :], 1, 1) for m in range(g)]
        if first:
            seen = lax.broadcasted_iota(jnp.int32, (own, own), 1) >= lax.broadcasted_iota(jnp.int32, (own, own), 0)
        weights, keeps = [], []
        for m, s in enumerate(scores):
            at = slice(m * own, (m + 1) * own)
            if first:
                s = jnp.where(seen, s, HIDDEN)
                top = s.max(axis=0, keepdims=True)
            else:
                old = top_s[h, :, at]
                top = jnp.maximum(old, s.max(axis=0, keepdims=True))
                keeps.append(jnp.exp2((old - top) * e2))
            top_s[h, :, at] = top
            weights.append(jnp.exp2((s - top) * e2).astype(BF16))
        for m, p in enumerate(weights):
            at = slice(m * own, (m + 1) * own)
            new = _dot(values, p, 1, 0)
            mix_s[h, :, at] = new if first else mix_s[h, :, at] * keeps[m] + new

    last_right, last_left = (me >= near) & (me < n - 1), (me == 0) | (me > half)

    def arrivals(r, h):
        def now(late):
            return None if r != near - 1 else ~late | (h < team)

        b = jnp.maximum(me - r, 0)

        @pl.when(comes_right(me, r))
        def _():
            right_copy(b, h, r - 1, None if r < half else 1).wait_recv()

        if r < half:
            send_right(r, h, start, now(last_right))

            @pl.when(comes_right(me, r))
            def _():
                attend(h, b, False)

        whole, part = comes_left(me, r)
        far = lax.rem(me + r, n)
        if whole is not False:
            @pl.when(whole)
            def _():
                left_copy(far, h, r - 1, None).wait_recv()

        @pl.when(part)
        def _():
            left_copy(far, h, r - 1, 0).wait_recv()

        if r < half:
            send_left(r, h, start, now(last_left))

        @pl.when((whole | part if r < half else part) & (me >= half))
        def _():
            attend(h, far, False)

    def queries(h, _):
        slot = lax.rem(h, 2)
        wait_tile(slot)

        @pl.when(h < kv - 1)
        def _():
            column_tile(wq_ref, jnp.minimum(h + 1, kv - 1), 1 - slot).start()

        @pl.when(h == kv - 1)
        def _():
            fetch_row_tile(0, 0)

        t = project(slot)
        for m in range(g):
            q_s[h, m * own : (m + 1) * own, :] = turned(t[:, m * HEAD : (m + 1) * HEAD].astype(F32))
        attend(h, me, True)
        arrivals(1, h)

    lax.fori_loop(0, kv, queries, None)
    for r in range(2, near):
        lax.fori_loop(0, kv, lambda h, _: arrivals(r, h), None)

    def group(which, _):
        base = which * team

        def middle(i, _):
            h = base + i
            arrivals(near, h)

            @pl.when(which < groups - 1)
            def _():
                kept = jnp.minimum(h + team, kv - 1)
                send_right(near - 1, kept, start, last_right)
                send_left(near - 1, kept, start, last_left)

        lax.fori_loop(0, team, middle, None)

        def last(i, _):
            h = base + i
            slot = lax.rem(h, 2)
            arrivals(half, h)
            for m in range(g):
                at = slice(m * own, (m + 1) * own)
                o = mix_s[h, :HEAD, at] * (1 / mix_s[h, HEAD : HEAD + 1, at])
                o_s[:, m * HEAD : (m + 1) * HEAD] = o.T.astype(BF16)
            wait_tile(slot)

            @pl.when(h < kv - 1)
            def _():
                fetch_row_tile(jnp.minimum(h + 1, kv - 1), 1 - slot)

            def out(c):
                return y_s[c] + _dot(o_s[...], w_s[slot, piece(c), :], 1, 0)

            def add(k, _):
                for m in range(parts // 2):
                    y_s[parts // 2 * k + m] = out(parts // 2 * k + m)

            def finish(k, _):
                for m in range(parts // 2):
                    c = parts // 2 * k + m
                    w_s[1 - slot, piece(c), :] = out(c).astype(BF16)
                    out_copy(c, 1 - slot).start()

            @pl.when(h < kv - 1)
            def _():
                lax.fori_loop(0, 2, add, None)

            @pl.when(h == kv - 1)
            def _():
                lax.fori_loop(0, 2, finish, None)

        lax.fori_loop(0, team, last, None)

    def out_copy(c, slot):
        return pltpu.make_async_copy(w_s.at[slot, piece(c), :], y_ref.at[:, piece(c)], y_sem.at[c])

    lax.fori_loop(0, groups, group, None)

    def settle(h, _):
        for s in range(half):
            send_right(s, h, lambda copy: copy.wait_send())
            send_left(s, h, lambda copy: copy.wait_send())

    lax.fori_loop(0, kv, settle, None)

    def stored(c, _):
        out_copy(c, 0).wait()

    lax.fori_loop(0, parts, stored, None)


def solution(mesh):
    n = mesh.shape["sp"]

    def step(x, gain, wq, wk, wv, wo):
        own, depth = x.shape
        kv = wk.shape[1] // HEAD
        g = wq.shape[1] // wk.shape[1]
        half = HEAD // 2
        turn = np.float32(THETA) ** (-np.arange(half, dtype=np.float32) / half)
        turn = jnp.asarray(np.concatenate([turn, turn])[None])
        hbm, vmem = pl.BlockSpec(memory_space=pl.ANY), pl.BlockSpec(memory_space=pltpu.VMEM)
        dma = pltpu.SemaphoreType.DMA
        return pl.pallas_call(
            functools.partial(_kernel, n, g, GROUPS),
            out_shape=jax.ShapeDtypeStruct((own, depth), BF16),
            in_specs=[hbm, vmem, vmem, hbm, hbm, hbm, hbm],
            out_specs=hbm,
            scratch_shapes=[
                pltpu.VMEM((own, HEAD), F32),
                pltpu.VMEM((own, HEAD), F32),
                pltpu.VMEM((own, depth), BF16),
                pltpu.VMEM((depth // TILE, own, TILE), F32),
                pltpu.VMEM((kv, g * own, HEAD), BF16),
                pltpu.VMEM((n, kv, 2, own, HEAD), BF16),
                pltpu.VMEM((kv, HEAD + 8, g * own), F32),
                pltpu.VMEM((kv, 1, g * own), F32),
                pltpu.VMEM((own, g * HEAD), BF16),
                pltpu.VMEM((2, depth, TILE), BF16),
                dma((2,)), dma, dma((depth // TILE,)),
                dma((n // 2, kv)), dma((n // 2, kv)), dma((n // 2, kv)), dma((n // 2, kv)),
            ],
            compiler_params=pltpu.CompilerParams(collective_id=0, has_side_effects=True, vmem_limit_bytes=67_043_328),
            cost_estimate=pl.CostEstimate(flops=2 * own * depth * (wq.shape[1] * 2 + wk.shape[1] * 2), bytes_accessed=2 * (2 * wq.size + 2 * wk.size), transcendentals=0),
        )(x, gain, turn, wq, wk, wv, wo)

    tokens, whole = P(("dp", "sp"), None), P(None, None)
    return jax.shard_map(
        step,
        mesh=mesh,
        in_specs=(tokens, P(None), whole, whole, whole, whole),
        out_specs=tokens,
        check_vma=False,
    )
```

```python
import functools

import jax
import jax.numpy as jnp
import numpy as np
from jax import lax
from jax.experimental import pallas as pl
from jax.experimental.pallas import tpu as pltpu
from jax.sharding import PartitionSpec as P

HEAD = 128
THETA = 10000
LOG2E = 1.4426950408889634
HIDDEN = -2e30
TILE = 512
F32, BF16 = jnp.float32, jnp.bfloat16


def _dot(a, b, ca, cb):
    return lax.dot_general(a, b, (((ca,), (cb,)), ((), ())), preferred_element_type=F32)


def _kernel(n, g, x_ref, gain_ref, turn_ref, wq_ref, wk_ref, wv_ref, wo_ref, y_ref,
            cos_s, sin_s, a_s, y_s, q_s, kv_s, mix_s, top_s, o_s, w_s, w_sem, x_sem, y_sem, sr_sem, sl_sem, rr_sem, rl_sem):
    own, depth = x_ref.shape
    kv = kv_s.shape[1]
    team = kv // 4
    sizes = (team, kv - 2 * team, team)
    half, near = n // 2, n // 2 - 1
    parts = depth // TILE
    scale = HEAD**-0.5
    e2 = scale * LOG2E
    me = lax.axis_index("sp")
    right, left = lax.rem(me + 1, n), lax.rem(me + n - 1, n)

    def column_tile(ref, t, slot):
        return pltpu.make_async_copy(ref.at[:, pl.ds(pl.multiple_of(t * TILE, TILE), TILE)], w_s.at[slot], w_sem.at[slot])

    def fetch_row_tile(h, slot):
        for c in range(parts):
            pltpu.make_async_copy(wo_ref.at[pl.ds(pl.multiple_of(h * TILE, TILE), TILE), c * TILE : (c + 1) * TILE],
                                  w_s.at[slot, c * TILE : (c + 1) * TILE, :], w_sem.at[slot]).start()

    def fetch_pair_tile(i, slot):
        for m in range(TILE // HEAD):
            cols = pl.ds(pl.multiple_of((2 * i + m // 2) * HEAD, HEAD), HEAD)
            pltpu.make_async_copy((wk_ref, wv_ref)[m % 2].at[:, cols], w_s.at[slot, :, m * HEAD : (m + 1) * HEAD], w_sem.at[slot]).start()

    def wait_tile(slot):
        column_tile(wq_ref, 0, slot).wait()

    for c in range(parts):
        pltpu.make_async_copy(x_ref.at[:, c * TILE : (c + 1) * TILE], w_s.at[1, c * TILE : (c + 1) * TILE, :], x_sem).start()
    fetch_pair_tile(0, 0)

    barrier = pltpu.get_barrier_semaphore()
    for neighbour in (left, right):
        pl.semaphore_signal(barrier, inc=1, device_id={"sp": neighbour}, device_id_type=pl.DeviceIdType.MESH)

    at = lax.broadcasted_iota(jnp.int32, (own, HEAD), 0) + me * own
    angle = at.astype(F32) * turn_ref[...]
    sine = jnp.sin(angle)
    cos_s[...] = jnp.cos(angle)
    sin_s[...] = jnp.where(lax.broadcasted_iota(jnp.int32, (own, HEAD), 1) < HEAD // 2, -sine, sine)

    pltpu.make_async_copy(wq_ref.at[:, :TILE], w_s.at[1], x_sem).wait()

    def piece(c):
        return pl.ds(pl.multiple_of(c * TILE, TILE), TILE)

    def squares(c, total):
        wide = w_s[1, piece(c), :].astype(F32)
        return total + (wide * wide).sum(-1, keepdims=True)

    total = lax.fori_loop(0, parts, squares, jnp.zeros((own, 1), F32))
    by = lax.rsqrt(total / depth + 1e-6)

    def norm(c, _):
        wide = w_s[1, piece(c), :].astype(F32)
        a_s[:, piece(c)] = (wide * by * gain_ref[piece(c)].astype(F32)[None]).astype(BF16)
        y_s[c] = wide

    lax.fori_loop(0, parts, norm, None)
    fetch_pair_tile(1, 1)

    pl.semaphore_wait(barrier, 2)

    def remote(b, h, to, send, receive, part):
        rows = slice(None) if part is None else slice(part * own // 2, (part + 1) * own // 2)
        ref = kv_s.at[b, h, :, rows, :]
        return pltpu.make_async_remote_copy(ref, ref, send, receive, device_id={"sp": to}, device_id_type=pl.DeviceIdType.MESH)

    def right_copy(b, h, at, part):
        return remote(b, h, right, sr_sem.at[at, h], rr_sem.at[at, h], part)

    def left_copy(b, h, at, part):
        return remote(b, h, left, sl_sem.at[at, h], rl_sem.at[at, h], part)

    def comes_right(i, s):
        return s <= i if s <= near else i >= half

    def comes_left(i, s):
        b = lax.rem(i + s, n)
        if s > near:
            return False, i >= half
        return (i != near) & (b < near), (i != near) & (b == near)

    def both(ok, also):
        return ok if also is None else ok & also

    def send_right(s, h, do, also=None):
        @pl.when(both((me < n - 1) & comes_right(me + 1, s + 1), also))
        def _():
            do(right_copy(jnp.maximum(me - s, 0), h, s, None if s < near else 1))

    def send_left(s, h, do, also=None):
        whole, part = comes_left(left, s + 1)
        b = lax.rem(me + s, n)
        if whole is not False:
            @pl.when(both(whole, also))
            def _():
                do(left_copy(b, h, s, None))

        @pl.when(both(part, also))
        def _():
            do(left_copy(b, h, s, 0))

    def start(copy):
        copy.start()

    def send_own(h):
        send_right(0, h, start)
        send_left(0, h, start)

    def turned(t):
        return (t * cos_s[...] + pltpu.roll(t, HEAD // 2, 1) * sin_s[...]).astype(BF16)

    def project(slot):
        return _dot(a_s[...], w_s[slot], 1, 0).astype(BF16)

    pair = TILE // HEAD // 2

    def keys_values(i, _):
        slot = lax.rem(i, 2)
        wait_tile(slot)
        for m in range(pair):
            h = i * pair + m
            t = _dot(a_s[...], w_s[slot, :, 2 * m * HEAD : 2 * (m + 1) * HEAD], 1, 0).astype(BF16)
            kv_s[me, h, 0] = turned(t[:, :HEAD].astype(F32))
            kv_s[me, h, 1] = t[:, HEAD:]
            send_own(h)

        @pl.when(i < kv // pair - 2)
        def _():
            fetch_pair_tile(jnp.minimum(i + 2, kv // pair - 1), slot)

        @pl.when(i == kv // pair - 2)
        def _():
            column_tile(wq_ref, 0, 0).start()

    lax.fori_loop(0, kv // pair, keys_values, None)

    ones = jnp.ones((8, own), BF16)

    def attend(h, b, first):
        keys, values = kv_s[b, h, 0], jnp.concatenate([kv_s[b, h, 1].T, ones], axis=0)
        scores = [_dot(keys, q_s[h, m * own : (m + 1) * own, :], 1, 1) for m in range(g)]
        if first:
            seen = lax.broadcasted_iota(jnp.int32, (own, own), 1) >= lax.broadcasted_iota(jnp.int32, (own, own), 0)
        weights, keeps = [], []
        for m, s in enumerate(scores):
            at = slice(m * own, (m + 1) * own)
            if first:
                s = jnp.where(seen, s, HIDDEN)
                top = s.max(axis=0, keepdims=True)
            else:
                old = top_s[h, :, at]
                top = jnp.maximum(old, s.max(axis=0, keepdims=True))
                keeps.append(jnp.exp2((old - top) * e2))
            top_s[h, :, at] = top
            weights.append(jnp.exp2((s - top) * e2).astype(BF16))
        for m, p in enumerate(weights):
            at = slice(m * own, (m + 1) * own)
            new = _dot(values, p, 1, 0)
            mix_s[h, :, at] = new if first else mix_s[h, :, at] * keeps[m] + new

    last_right, last_left = (me >= near) & (me < n - 1), (me == 0) | (me > half)

    def arrivals(r, h):
        def now(late):
            return None if r != near - 1 else ~late | (h < team)

        b = jnp.maximum(me - r, 0)

        @pl.when(comes_right(me, r))
        def _():
            right_copy(b, h, r - 1, None if r < half else 1).wait_recv()

        if r < half:
            send_right(r, h, start, now(last_right))

            @pl.when(comes_right(me, r))
            def _():
                attend(h, b, False)

        whole, part = comes_left(me, r)
        far = lax.rem(me + r, n)
        if whole is not False:
            @pl.when(whole)
            def _():
                left_copy(far, h, r - 1, None).wait_recv()

        @pl.when(part)
        def _():
            left_copy(far, h, r - 1, 0).wait_recv()

        if r < half:
            send_left(r, h, start, now(last_left))

        @pl.when((whole | part if r < half else part) & (me >= half))
        def _():
            attend(h, far, False)

    def queries(h, _):
        slot = lax.rem(h, 2)
        wait_tile(slot)

        @pl.when(h < kv - 1)
        def _():
            column_tile(wq_ref, jnp.minimum(h + 1, kv - 1), 1 - slot).start()

        @pl.when(h == kv - 1)
        def _():
            fetch_row_tile(0, 0)

        t = project(slot)
        for m in range(g):
            q_s[h, m * own : (m + 1) * own, :] = turned(t[:, m * HEAD : (m + 1) * HEAD].astype(F32))
        attend(h, me, True)
        arrivals(1, h)

    lax.fori_loop(0, kv, queries, None)
    for r in range(2, near):
        lax.fori_loop(0, kv, lambda h, _: arrivals(r, h), None)

    def group(which, _):
        base = jnp.where(which == 0, 0, jnp.where(which == 1, sizes[0], sizes[0] + sizes[1]))
        size = jnp.where(which == 1, sizes[1], sizes[0])
        following = jnp.where(which == 0, sizes[1], jnp.where(which == 1, sizes[2], 0))

        def middle(i, _):
            h = base + i
            arrivals(near, h)

            for m in range(2):
                kept = lax.div(following * i, size) + m

                @pl.when(kept < lax.div(following * (i + 1), size))
                def _():
                    at = jnp.minimum(base + size + kept, kv - 1)
                    send_right(near - 1, at, start, last_right)
                    send_left(near - 1, at, start, last_left)

        lax.fori_loop(0, size, middle, None)

        def last(i, _):
            h = base + i
            slot = lax.rem(h, 2)
            arrivals(half, h)
            wait_tile(slot)

            @pl.when(h < kv - 1)
            def _():
                fetch_row_tile(jnp.minimum(h + 1, kv - 1), 1 - slot)

            def products():
                share = []
                for m in range(g):
                    at = slice(m * own, (m + 1) * own)
                    share.append((mix_s[h, :HEAD, at] * (1 / mix_s[h, HEAD : HEAD + 1, at])).astype(BF16).T)
                o_s[...] = jnp.concatenate(share, axis=1)
                for c in range(parts):
                    yield c, y_s[c] + _dot(o_s[...], w_s[slot, c * TILE : (c + 1) * TILE, :], 1, 0)

            @pl.when(h < kv - 1)
            def _():
                for c, y in products():
                    y_s[c] = y

            @pl.when(h == kv - 1)
            def _():
                for c, y in products():
                    w_s[1 - slot, c * TILE : (c + 1) * TILE, :] = y.astype(BF16)
                    out_copy(c, 1 - slot).start()

        lax.fori_loop(0, size, last, None)

    def out_copy(c, slot):
        return pltpu.make_async_copy(w_s.at[slot, piece(c), :], y_ref.at[:, piece(c)], y_sem.at[c])

    lax.fori_loop(0, len(sizes), group, None)

    def settle(h, _):
        for s in range(half):
            send_right(s, h, lambda copy: copy.wait_send())
            send_left(s, h, lambda copy: copy.wait_send())

    lax.fori_loop(0, kv, settle, None)

    def stored(c, _):
        out_copy(c, 0).wait()

    lax.fori_loop(0, parts, stored, None)


def solution(mesh):
    n = mesh.shape["sp"]

    def step(x, gain, wq, wk, wv, wo):
        own, depth = x.shape
        kv = wk.shape[1] // HEAD
        g = wq.shape[1] // wk.shape[1]
        half = HEAD // 2
        turn = np.float32(THETA) ** (-np.arange(half, dtype=np.float32) / half)
        turn = jnp.asarray(np.concatenate([turn, turn])[None])
        hbm, vmem = pl.BlockSpec(memory_space=pl.ANY), pl.BlockSpec(memory_space=pltpu.VMEM)
        dma = pltpu.SemaphoreType.DMA
        return pl.pallas_call(
            functools.partial(_kernel, n, g),
            out_shape=jax.ShapeDtypeStruct((own, depth), BF16),
            in_specs=[hbm, vmem, vmem, hbm, hbm, hbm, hbm],
            out_specs=hbm,
            scratch_shapes=[
                pltpu.VMEM((own, HEAD), F32),
                pltpu.VMEM((own, HEAD), F32),
                pltpu.VMEM((own, depth), BF16),
                pltpu.VMEM((depth // TILE, own, TILE), F32),
                pltpu.VMEM((kv, g * own, HEAD), BF16),
                pltpu.VMEM((n, kv, 2, own, HEAD), BF16),
                pltpu.VMEM((kv, HEAD + 8, g * own), F32),
                pltpu.VMEM((kv, 1, g * own), F32),
                pltpu.VMEM((own, g * HEAD), BF16),
                pltpu.VMEM((2, depth, TILE), BF16),
                dma((2,)), dma, dma((depth // TILE,)),
                dma((n // 2, kv)), dma((n // 2, kv)), dma((n // 2, kv)), dma((n // 2, kv)),
            ],
            compiler_params=pltpu.CompilerParams(collective_id=0, has_side_effects=True, vmem_limit_bytes=67_043_328),
            cost_estimate=pl.CostEstimate(flops=2 * own * depth * (wq.shape[1] * 2 + wk.shape[1] * 2), bytes_accessed=2 * (2 * wq.size + 2 * wk.size), transcendentals=0),
        )(x, gain, turn, wq, wk, wv, wo)

    tokens, whole = P(("dp", "sp"), None), P(None, None)
    return jax.shard_map(
        step,
        mesh=mesh,
        in_specs=(tokens, P(None), whole, whole, whole, whole),
        out_specs=tokens,
        check_vma=False,
    )
```
